32 devices in a mesh: groups: 2 (over y), px: 16 (over z, x, core).
Axes of the slice: x: 2, y: 2, z: 4, core: 2. Of those that a mesh axis runs over, the one named last changes fastest.
Arguments:
- features: bfloat16 [32, 256, 256, 256], P(None, ('groups', 'px')), parts along dimension 1, may hold values from -6 to 6
- pointwise_weight: bfloat16 [32, 32], replicated, may hold values from -1 to 1
- pointwise_bias: float32 [32], replicated, may hold values from -3 to 3
- spectral_weight: float32 [2, 32, 32, 16384], P(None, None, None, 'px'), may hold values from -6 to 6
Outputs:
- updated: bfloat16 [32, 256, 256, 256], P(None, ('groups', 'px')), parts along dimension 1
The draws below stay inside these ranges and needn't reach their ends.
There are 2 independent parts, one for each index of `groups`. The reference program is written for one: setup_inputs(seed, part) draws one part's arguments, and reference() takes and returns one part's arrays. A program takes and returns all parts, laid end to end along the dimension named above; an argument that names none is the same for every part. Nothing has to cross between parts.
All inputs are finite; a program needn't handle non-finite values.
Results may differ from the reference program's by a relative error of at most 0.0025.
Values sent between devices are 32-bit elements; how exact they have to be, the bound alone decides.
A program may use at most 256 MiB of HBM per device.

```python
import math
import jax
import jax.numpy as jnp
from jax import lax

C = 32
X = 128
Y = 256
Z = 256
KX = 32
KY = 32
KZ = 16
MODES = 16384


def steps_of(key, shape, cuts, least, largest):
    level = 1.0
    for axis_at, parts in cuts:
        draws = jax.random.uniform(jax.random.fold_in(jax.random.fold_in(key, 6), axis_at), (parts,), jnp.float32, least / len(cuts), largest / len(cuts))
        level = level * jnp.repeat(jnp.exp(draws), shape[axis_at] // parts).reshape((-1,) + (1,) * (len(shape) - 1 - axis_at))
    return level


def gaussian(key, dims, scale, most, cuts=(), kind=jnp.bfloat16):
    drawn = scale * jax.random.normal(key, dims, jnp.float32)
    if cuts:
        drawn = drawn * steps_of(key, dims, cuts, -0.22, 0.18)
    return jnp.clip(drawn, -most, most).astype(kind)


def setup_inputs(seed: int = 0, part: int = 0) -> dict:
    seeds = jax.random.split(jax.random.key(seed), 5)
    own_keys = jax.random.split(jax.random.fold_in(seeds[4], part), 5)
    features = gaussian(own_keys[0], (C, X, Y, Z), 1.0, 6.0, ((1, 16),))
    pointwise_weight = gaussian(seeds[1], (C, C), C ** -0.5, 1.0)
    pointwise_bias = gaussian(seeds[2], (C,), 0.5, 3.0, (), jnp.float32)
    spectral_weight = gaussian(seeds[3], (2, C, C, MODES), 1.0, 6.0, ((3, 16),), jnp.float32)
    return {"features": features, "pointwise_weight": pointwise_weight, "pointwise_bias": pointwise_bias, "spectral_weight": spectral_weight}


TWO_PI = 2.0 * math.pi


def signed_modes(number):
    ladder = jnp.arange(number, dtype=jnp.int32)
    return jnp.where(ladder < number // 2, ladder, ladder - number)


def phase_table(positions, frequency, length):
    product = (positions[:, None] * frequency[None, :]) % length
    return product.astype(jnp.float32) * (TWO_PI / length)


def forward_table(positions):
    x_phase = phase_table(positions, signed_modes(KX), X)
    cosine = jnp.cos(x_phase)
    sine = jnp.sin(x_phase)
    return jnp.stack([jnp.stack([cosine, -sine], axis=1), jnp.stack([sine, cosine], axis=1)], axis=0)


def inverse_table(positions):
    x_phase = phase_table(positions, signed_modes(KX), X)
    cosine = jnp.cos(x_phase)
    sine = jnp.sin(x_phase)
    return jnp.stack([jnp.stack([cosine, sine], axis=1), jnp.stack([-sine, cosine], axis=1)], axis=0)


def spectra_local(features):
    channels = features.shape[0]
    planes = features.shape[1]
    z_phase = phase_table(jnp.arange(Z, dtype=jnp.int32), jnp.arange(KZ, dtype=jnp.int32), Z)
    z_table = jnp.concatenate([jnp.cos(z_phase), -jnp.sin(z_phase)], axis=1).astype(jnp.bfloat16)
    flat = features.reshape(channels * planes * Y, Z)
    along_z = jnp.dot(flat, z_table, preferred_element_type=jnp.float32)
    stacked = along_z.reshape(channels, planes, Y, 2, KZ).transpose(3, 0, 1, 4, 2)
    y_phase = phase_table(jnp.arange(Y, dtype=jnp.int32), signed_modes(KY), Y)
    cosine = jnp.einsum('rcxky,yj->rcxjk', stacked, jnp.cos(y_phase), precision=lax.Precision.HIGHEST)
    sine = jnp.einsum('rcxky,yj->rcxjk', stacked, jnp.sin(y_phase), precision=lax.Precision.HIGHEST)
    real_part = cosine[0] + sine[1]
    imag_part = cosine[1] - sine[0]
    return jnp.stack([real_part, imag_part]).reshape(2, channels, planes, KY * KZ)


def along_first(partial_value, table):
    return jnp.einsum('rcxq,rxsk->qsck', partial_value, table, precision=lax.Precision.HIGHEST)


def contract(left, right):
    return jnp.einsum('im,iom->om', left, right, precision=lax.Precision.HIGHEST)


def mix_modes(spectrum, weights):
    real_part = contract(spectrum[0], weights[0]) - contract(spectrum[1], weights[1])
    imag_part = contract(spectrum[0], weights[1]) + contract(spectrum[1], weights[0])
    return jnp.stack([real_part, imag_part])


def back_first(blended, table):
    return jnp.einsum('rcqk,rxsk->scxq', blended, table, precision=lax.Precision.HIGHEST)


def finish_planes(spread, features, pointwise_weight, pointwise_bias):
    channels = features.shape[0]
    planes = features.shape[1]
    folded = spread.reshape(2, channels, planes, KY, KZ)
    y_phase = phase_table(jnp.arange(Y, dtype=jnp.int32), signed_modes(KY), Y)
    cosine = jnp.einsum('rcxjk,yj->rcxky', folded, jnp.cos(y_phase), precision=lax.Precision.HIGHEST)
    sine = jnp.einsum('rcxjk,yj->rcxky', folded, jnp.sin(y_phase), precision=lax.Precision.HIGHEST)
    halves = jnp.concatenate([cosine[0] - sine[1], sine[0] + cosine[1]], axis=2)
    z_phase = phase_table(jnp.arange(Z, dtype=jnp.int32), jnp.arange(KZ, dtype=jnp.int32), Z)
    factor = jnp.where(jnp.arange(KZ, dtype=jnp.int32) == 0, 1.0, 2.0).astype(jnp.float32) / (1.0 * X * Y * Z)
    z_table = jnp.concatenate([factor[:, None] * jnp.cos(z_phase).T, -factor[:, None] * jnp.sin(z_phase).T], axis=0)
    spectral = jnp.einsum('cxjy,jz->cxyz', halves, z_table, precision=lax.Precision.HIGHEST)
    linear = jnp.dot(pointwise_weight, features.reshape(channels, planes * Y * Z), preferred_element_type=jnp.float32).reshape(channels, planes, Y, Z)
    summed = spectral + linear + pointwise_bias[:, None, None, None]
    inner = 0.7978845608 * (summed + 0.044715 * summed * summed * summed)
    return (0.5 * summed * (1.0 + jnp.tanh(inner))).astype(jnp.bfloat16)


def reference(features, pointwise_weight, pointwise_bias, spectral_weight):
    indices = jnp.arange(X, dtype=jnp.int32)

    def forward_plane(plane_index):
        return spectra_local(lax.dynamic_slice_in_dim(features, plane_index, 1, 1))[:, :, 0, :]

    partial_value = jnp.moveaxis(lax.map(forward_plane, indices), 0, 2)
    spectrum = along_first(partial_value, forward_table(indices)).transpose(1, 2, 0, 3).reshape(2, C, KY * KZ * KX)
    blended = mix_modes(spectrum, spectral_weight).reshape(2, C, KY * KZ, KX)
    spread = back_first(blended, inverse_table(indices))

    def finish_plane(plane_index):
        return finish_planes(lax.dynamic_slice_in_dim(spread, plane_index, 1, 2), lax.dynamic_slice_in_dim(features, plane_index, 1, 1), pointwise_weight, pointwise_bias)[:, 0]

    return jnp.moveaxis(lax.map(finish_plane, indices), 0, 1)
```

```python
import functools
import math

import jax
import jax.numpy as jnp
import numpy as np
from jax import lax
from jax.experimental import pallas as pl
from jax.experimental.pallas import tpu as pltpu
from jax.sharding import PartitionSpec as P

KX = 32
KY = 32
KZ = 16
LANES = 128
PACK = LANES // KZ
QUAD = 4

TWO_PI = 2.0 * math.pi


def signed_modes(number):
    ladder = np.arange(number)
    return np.where(ladder < number // 2, ladder, ladder - number)


def phase_table(length, frequency):
    product = np.arange(length)[:, None] * frequency[None, :] % length
    return product.astype(np.float32) * np.float32(TWO_PI / length)


def rounded(table):
    return np.asarray(table).astype(jnp.bfloat16)


def split(table):
    high = rounded(table)
    return high, rounded(table - high.astype(np.float32))


def forward_table(length):
    phase = phase_table(length, signed_modes(KX))
    cosine, sine = np.cos(phase), np.sin(phase)
    return np.stack([np.stack([cosine, -sine], axis=1), np.stack([sine, cosine], axis=1)], axis=0)


def inverse_table(length):
    phase = phase_table(length, signed_modes(KX))
    cosine, sine = np.cos(phase), np.sin(phase)
    return np.stack([np.stack([cosine, sine], axis=1), np.stack([-sine, cosine], axis=1)], axis=0)


def halves(value):
    high = value.astype(jnp.bfloat16)
    return high, (value - high.astype(jnp.float32)).astype(jnp.bfloat16)


def product(left, right):
    return jnp.dot(left, right, preferred_element_type=jnp.float32)


def chosen(table, axis, width, count, which):
    place = lax.broadcasted_iota(jnp.int32, table.shape, axis) // width % count
    return jnp.where(place == which, table.astype(jnp.float32), 0.0).astype(jnp.bfloat16)


def whole(*shape):
    return pl.BlockSpec(shape, lambda *step: (0,) * len(shape))


def others(parts, act):
    me = lax.axis_index("px")

    def one(k, carry):
        act(lax.rem(me + k, parts))
        return carry

    lax.fori_loop(1, parts, one, 0)


def greet(parts):
    barrier = pltpu.get_barrier_semaphore()
    others(parts, lambda to: pl.semaphore_signal(barrier, inc=1, device_id={"px": to}))


def greeted(parts):
    pl.semaphore_wait(pltpu.get_barrier_semaphore(), parts - 1)


def share(parts, sent, out, at, sems):
    me = lax.axis_index("px")
    send, receive, local = sems

    def put(to):
        pltpu.make_async_remote_copy(
            src_ref=sent.at[to, at], dst_ref=out.at[me, at], send_sem=send, recv_sem=receive, device_id={"px": to}
        ).start()

    others(parts, put)
    pltpu.make_async_copy(sent.at[me, at], out.at[me, at], local).start()


def settle(parts, sent, out, sems):
    send, receive, local = sems
    pltpu.make_async_copy(sent.at[0], out.at[0], local).wait()
    most = pl.ds(0, parts - 1)
    every = pltpu.make_async_remote_copy(
        src_ref=sent.at[most], dst_ref=out.at[most], send_sem=send, recv_sem=receive,
        device_id={"px": lax.rem(lax.axis_index("px") + 1, parts)},
    )
    every.wait_send()
    every.wait_recv()


def spread_z(base_ref, z):
    depth = base_ref.shape[0]
    for c in range(PACK):
        z[c * depth : (c + 1) * depth] = chosen(base_ref[...], 1, KZ, PACK, c)


def plane_spectra(f_ref, z, y_ref, keep):
    groups = f_ref.shape[0] // PACK
    depth = f_ref.shape[3]
    for pair in range(0, groups, 2):
        along = [0.0, 0.0]
        for c in range(PACK):
            for n in range(2):
                along[n] += product(f_ref[(pair + n) * PACK + c, 0], z[c * depth : (c + 1) * depth])
        for n in range(2):
            g = pair + n
            high, low = halves(along[n])
            both = product(y_ref[...], high)
            rest = product(y_ref[: 2 * KY], low)
            total = both[: 2 * KY] + both[2 * KY :] + rest
            cosine, sine = total[:KY], total[KY:]
            keep(g, cosine[:, :LANES] + sine[:, LANES:])
            keep(groups + g, cosine[:, LANES:] - sine[:, :LANES])


def forward_kernel(f_ref, base_ref, y_ref, out_ref, z):
    @pl.when(pl.program_id(0) == 0)
    def start():
        spread_z(base_ref, z)

    def keep(row, value):
        out_ref[:, 0, row, :] = value

    plane_spectra(f_ref, z, y_ref, keep)


def forward_share_kernel(f_ref, base_ref, y_ref, out_ref, z, sent, send, receive, local):
    x = pl.program_id(0)
    parts, _, held_y = sent.shape[:3]

    @pl.when(x == 0)
    def start():
        greet(parts)
        spread_z(base_ref, z)

    def keep(row, value):
        sent[:, pl.ds(x, 1), :, row, :] = value.reshape(parts, 1, held_y, LANES)

    plane_spectra(f_ref, z, y_ref, keep)

    @pl.when(x == 0)
    def ready():
        greeted(parts)

    share(parts, sent, out_ref, x, (send, receive, local))

    @pl.when(x == pl.num_programs(0) - 1)
    def end():
        settle(parts, sent, out_ref, (send, receive, local))


def spectra(parts, features):
    channels, planes, height, depth = features.shape
    rows = 2 * channels // PACK
    y_phase = phase_table(height, signed_modes(KY)).T
    high, low = split(np.concatenate([np.cos(y_phase), np.sin(y_phase)], axis=0))
    z_phase = phase_table(depth, np.arange(KZ))
    base = rounded(np.concatenate([np.tile(np.cos(z_phase), (1, PACK)), np.tile(-np.sin(z_phase), (1, PACK))], axis=1))
    y_table = np.concatenate([high, low], axis=0)
    call = dict(
        grid=(planes,),
        in_specs=[
            pl.BlockSpec((channels, 1, height, depth), lambda x: (0, x, 0, 0)),
            whole(*base.shape),
            whole(*y_table.shape),
        ],
    )
    z = pltpu.VMEM((PACK * depth, 2 * LANES), jnp.bfloat16)
    if parts is None:
        kernel, shape = forward_kernel, (KY, planes, rows, LANES)
        call |= dict(
            out_specs=pl.BlockSpec((KY, 1, rows, LANES), lambda x: (0, x, 0, 0)),
            scratch_shapes=[z],
            compiler_params=pltpu.CompilerParams(vmem_limit_bytes=48 << 20),
            name="forward_planes",
        )
    else:
        kernel, shape = forward_share_kernel, (parts, planes, KY // parts, rows, LANES)
        call |= dict(
            out_specs=pl.BlockSpec(memory_space=pl.ANY),
            scratch_shapes=[z, pltpu.VMEM(shape, jnp.float32)] + [pltpu.SemaphoreType.DMA] * 3,
            compiler_params=pltpu.CompilerParams(vmem_limit_bytes=48 << 20, collective_id=0, has_side_effects=True),
            name="forward_share",
        )
    out_shape = jax.ShapeDtypeStruct(shape, jnp.float32)
    return pl.pallas_call(kernel, out_shape=out_shape, **call)(features, jnp.asarray(base), jnp.asarray(y_table))


def contract(left, right):
    return jnp.einsum("im,iom->om", left, right, precision=lax.Precision.HIGHEST)


def mix_modes(spectrum, weights):
    real_part = contract(spectrum[0], weights[0]) - contract(spectrum[1], weights[1])
    imag_part = contract(spectrum[0], weights[1]) + contract(spectrum[1], weights[0])
    return jnp.stack([real_part, imag_part])


def spectrum_table(length):
    table = np.broadcast_to(forward_table(length)[:, :, :, None, :], (2, length, 2, QUAD, KX))
    return split(table.reshape(2 * length, 2 * QUAD * KX))


def planes_table(length):
    table = inverse_table(length).transpose(0, 3, 2, 1)
    table = np.broadcast_to(table[:, None], (2, QUAD, KX, 2, length))
    return split(table.reshape(2 * QUAD * KX, 2 * length))


def modes_kernel(g_ref, fhigh_ref, flow_ref, ihigh_ref, ilow_ref, w_ref, out_ref, *scratch):
    fhigh, flow, ihigh, ilow, turned, spectrum, blended, placed, sent, send, receive, local = scratch
    parts, planes, held_y, rows, _ = g_ref.shape
    length = parts * planes
    channels = w_ref.shape[1]
    quads = KZ // QUAD
    groups = rows // 2
    here = pl.program_id(0)

    @pl.when(here == 0)
    def along_x():
        greet(parts)
        for q in range(QUAD):
            at = slice(q * 2 * length, (q + 1) * 2 * length)
            fhigh[at], flow[at] = chosen(fhigh_ref[...], 1, KX, QUAD, q), chosen(flow_ref[...], 1, KX, QUAD, q)
            ihigh[:, at], ilow[:, at] = chosen(ihigh_ref[...], 0, KX, QUAD, q), chosen(ilow_ref[...], 0, KX, QUAD, q)
        for j in range(held_y):
            for r in range(2):
                for g in range(groups):
                    tile = g_ref[:, :, j, r * groups + g, :].reshape(length, LANES)
                    turned[j, r, g * LANES : (g + 1) * LANES, :] = tile.T
        for b in range(held_y * quads):
            j, base = b // quads, b % quads * QUAD
            pieces = [turned[j, r, pl.ds(base + q, channels, stride=KZ), :] for q in range(QUAD) for r in range(2)]
            high, low = halves(jnp.concatenate(pieces, axis=1))
            spectrum[b] = product(high, fhigh[...]) + product(high, flow[...]) + product(low, fhigh[...])

    def mix(i, total):
        real, imag = total
        row = spectrum[here, pl.ds(i, 1), :]
        s_real, s_imag = row[:, :LANES], row[:, LANES:]
        w_real, w_imag = w_ref[0, i], w_ref[1, i]
        return real + (s_real * w_real - s_imag * w_imag), imag + (s_real * w_imag + s_imag * w_real)

    zero = jnp.zeros((channels, LANES), jnp.float32)
    real, imag = lax.fori_loop(0, channels, mix, (zero, zero), unroll=4)
    blended[here, :, :LANES] = real
    blended[here, :, LANES:] = imag

    for j in range(held_y):

        @pl.when(here == (j + 1) * quads - 1)
        def back_along_x():
            high, low = halves(blended[j * quads : (j + 1) * quads].reshape(quads * channels, 2 * LANES))
            value = product(high, ihigh[...]) + product(high, ilow[...]) + product(low, ihigh[...])
            for b in range(quads):
                for q in range(QUAD):
                    for r in range(2):
                        at = (q * 2 + r) * length
                        row = pl.ds(r * KZ + b * QUAD + q, channels, stride=2 * KZ)
                        placed[j, row, :] = value[b * channels : (b + 1) * channels, at : at + length]
            for h in range(sent.shape[3]):
                tile = placed[j, h * LANES : (h + 1) * LANES, :].T
                sent[:, j, :, h, :] = tile.reshape(parts, planes, LANES)
            if j == 0:
                greeted(parts)
            share(parts, sent, out_ref, j, (send, receive, local))
            if j == held_y - 1:
                settle(parts, sent, out_ref, (send, receive, local))


def mix_on_device(gathered, spectral_weight):
    parts, planes, held_y, rows, _ = gathered.shape
    length = parts * planes
    channels = spectral_weight.shape[1]
    blocks = held_y * KZ // QUAD
    tables = (*spectrum_table(length), *planes_table(length))
    packs = channels * 2 * KZ // LANES
    shape = (parts, held_y, planes, packs, LANES)
    wide = QUAD * 2 * length
    return pl.pallas_call(
        modes_kernel,
        grid=(blocks,),
        out_shape=jax.ShapeDtypeStruct(shape, jnp.float32),
        in_specs=[whole(*gathered.shape)]
        + [whole(*table.shape) for table in tables]
        + [pl.BlockSpec((2, channels, channels, LANES), lambda b: (0, 0, 0, b))],
        out_specs=pl.BlockSpec(memory_space=pl.ANY),
        scratch_shapes=[pltpu.VMEM((wide, 2 * LANES), jnp.bfloat16)] * 2
        + [pltpu.VMEM((2 * LANES, wide), jnp.bfloat16)] * 2
        + [
            pltpu.VMEM((held_y, 2, channels * KZ, length), jnp.float32),
            pltpu.VMEM((blocks, channels, 2 * LANES), jnp.float32),
            pltpu.VMEM((blocks, channels, 2 * LANES), jnp.float32),
            pltpu.VMEM((held_y, channels * 2 * KZ, length), jnp.float32),
            pltpu.VMEM(shape, jnp.float32),
        ]
        + [pltpu.SemaphoreType.DMA] * 3,
        compiler_params=pltpu.CompilerParams(vmem_limit_bytes=40 << 20, collective_id=1, has_side_effects=True),
        name="mix_share",
    )(gathered, *map(jnp.asarray, tables), spectral_weight)


def inverse_kernel(f_ref, q_ref, w_ref, left_ref, right_ref, zhigh_ref, zlow_ref, y_ref, bias_ref, out_ref, *scratch):
    mix, z, linear, other, waves = scratch
    channels, _, height, depth = f_ref.shape
    rows_each = height // channels
    packs = LANES // (2 * KZ)
    stacks = channels // packs
    step = pl.program_id(0)

    @pl.when(step == 0)
    def start():
        tall = product(left_ref[...], w_ref[...]).astype(jnp.bfloat16)
        wide = product(tall, right_ref[...])
        row = lax.broadcasted_iota(jnp.int32, wide.shape, 0)
        column = lax.broadcasted_iota(jnp.int32, wide.shape, 1)
        mix[...] = jnp.where(row % rows_each == column % rows_each, 0.5 * wide, 0.0).astype(jnp.bfloat16)
        z[...] = jnp.zeros_like(z)
        for k in range(packs):
            at = k * 2 * KZ
            z[k, at : at + 2 * KZ] = zhigh_ref[...]
            z[k, LANES + at : LANES + at + 2 * KZ] = zhigh_ref[...]
            z[k, 2 * LANES + at : 2 * LANES + at + 2 * KZ] = zlow_ref[...]

    def along_z():
        modes = jnp.concatenate([q_ref[:, :, 0, h, :].reshape(KY, LANES) for h in range(stacks)], axis=0)
        high, low = halves(modes)
        modes = jnp.concatenate([high, low, high], axis=1)
        first = lax.broadcasted_iota(jnp.int32, (KY, depth), 0) == 0
        for k in range(packs):
            value = product(modes, z[k])
            for h in range(stacks):
                c = h * packs + k
                part = value[h * KY : (h + 1) * KY]
                real = part[:, :depth] + jnp.where(first, 0.5 * bias_ref[c], 0.0)
                imag = part[:, depth:]
                waves[c, :KY], waves[c, 2 * KY : 3 * KY] = halves(real)
                waves[c, KY : 2 * KY], waves[c, 3 * KY :] = halves(imag)

    def pointwise(t, into):
        rows = pl.ds(pl.multiple_of(t * rows_each, rows_each), rows_each)
        local = f_ref[:, 0, rows, :].reshape(height, depth)
        into[:, rows, :] = product(mix[...], local).reshape(channels, rows_each, depth)

    def finish(c, held):
        wave = waves[c]
        stack = jnp.concatenate([wave, wave[: 2 * KY]], axis=0)
        half = product(y_ref[...], stack) + held[c]
        inner = half * (2.0 * 0.7978845608 + (8.0 * 0.7978845608 * 0.044715) * (half * half))
        out_ref[c, 0] = (half + half * jnp.tanh(inner)).astype(jnp.bfloat16)

    def work(into, held):
        along_z()

        def both(t, carry):
            pointwise(t, into)
            finish(t, held)
            return carry

        lax.fori_loop(0, channels, both, 0, unroll=8)

    @pl.when(step % 2 == 0)
    def even():
        work(linear, other)

    @pl.when(step % 2 == 1)
    def odd():
        work(other, linear)


def finish_planes(modes, features, pointwise_weight, pointwise_bias, cells):
    channels, planes, height, depth = features.shape
    owners, held_y, _, stacks, _ = modes.shape
    y_phase = phase_table(height, signed_modes(KY))
    high, low = split(np.concatenate([np.cos(y_phase), -np.sin(y_phase)], axis=1))
    y_table = np.concatenate([high, high, low], axis=1)
    z_phase = phase_table(depth, np.arange(KZ)).T
    factor = (0.5 * np.where(np.arange(KZ) == 0, 1.0, 2.0) / cells).astype(np.float32)[:, None]
    cosine, sine = factor * np.cos(z_phase), factor * np.sin(z_phase)
    z_high, z_low = split(np.block([[cosine, sine], [-sine, cosine]]))
    left = rounded(np.repeat(np.eye(channels, dtype=np.float32), height // channels, axis=0))
    plane = (channels, 1, height, depth)
    packs = LANES // (2 * KZ)
    return pl.pallas_call(
        inverse_kernel,
        grid=(planes + 1,),
        out_shape=jax.ShapeDtypeStruct(features.shape, jnp.bfloat16),
        in_specs=[
            pl.BlockSpec(plane, lambda x: (0, jnp.minimum(x, planes - 1), 0, 0)),
            pl.BlockSpec((owners, held_y, 1, stacks, LANES), lambda x: (0, 0, jnp.maximum(x - 1, 0), 0, 0)),
            whole(channels, channels),
            whole(height, channels),
            whole(channels, height),
            whole(*z_high.shape),
            whole(*z_low.shape),
            whole(*y_table.shape),
            pl.BlockSpec(memory_space=pltpu.SMEM),
        ],
        out_specs=pl.BlockSpec(plane, lambda x: (0, jnp.maximum(x - 1, 0), 0, 0)),
        scratch_shapes=[
            pltpu.VMEM((height, height), jnp.bfloat16),
            pltpu.VMEM((packs, 3 * LANES, 2 * depth), jnp.bfloat16),
            pltpu.VMEM((channels, height, depth), jnp.float32),
            pltpu.VMEM((channels, height, depth), jnp.float32),
            pltpu.VMEM((channels, 4 * KY, depth), jnp.bfloat16),
        ],
        compiler_params=pltpu.CompilerParams(vmem_limit_bytes=56 << 20),
        name="inverse_planes",
    )(
        features, modes, pointwise_weight, jnp.asarray(left), jnp.asarray(left.T), jnp.asarray(z_high),
        jnp.asarray(z_low), jnp.asarray(y_table), pointwise_bias,
    )


def by_einsum(parts, features, spectral_weight):
    channels, planes, height, depth = features.shape
    length = planes * parts
    held_y = max(KY // parts, 1)
    cuts = parts * held_y // KY
    held_z = KZ // cuts
    packs = LANES // (2 * KZ)
    exact = functools.partial(jnp.einsum, precision=lax.Precision.HIGHEST)
    exchange = functools.partial(lax.all_to_all, axis_name="px", split_axis=0, concat_axis=0, tiled=True)

    sent = spectra(None, features)
    sent = sent.reshape(KY, planes, 2 * channels, cuts, held_z).transpose(0, 3, 1, 2, 4)
    sent = sent.reshape(parts, held_y * planes * 2 * channels * held_z // LANES, LANES)
    gathered = exchange(sent).reshape(parts, held_y, planes, 2, channels, held_z)
    table = jnp.asarray(forward_table(length).reshape(2, parts, planes, 2, KX))
    spectrum = exact("sjprck,rsptm->tcjkm", gathered, table)
    blended = mix_modes(spectrum.reshape(2, channels, held_y * held_z * KX), spectral_weight)
    blended = blended.reshape(2, channels, held_y, held_z, KX)
    table = jnp.asarray(inverse_table(length).reshape(2, parts, planes, 2, KX))
    sent = exact("rcjkm,rsptm->spjtck", blended, table)
    sent = sent.reshape(parts, held_y * planes * 2 * channels * held_z // LANES, LANES)
    spread = exchange(sent).reshape(KY // held_y, cuts, planes, held_y, 2, channels // packs, packs, held_z)
    modes = spread.transpose(0, 3, 2, 5, 6, 4, 1, 7)
    return modes.reshape(KY // held_y, held_y, planes, channels // packs, LANES)


def on_device(parts, features, pointwise_weight, pointwise_bias, spectral_weight):
    channels, planes, height, depth = features.shape
    length = planes * parts
    if KY % parts == 0 and length == LANES:
        modes = mix_on_device(spectra(parts, features), spectral_weight)
    else:
        modes = by_einsum(parts, features, spectral_weight)
    return finish_planes(
        modes, features, pointwise_weight, pointwise_bias, 1.0 * length * height * depth
    )


def solution(mesh):
    in_specs = (P(None, ("groups", "px"), None, None), P(), P(), P(None, None, None, "px"))
    out_specs = P(None, ("groups", "px"), None, None)
    return jax.shard_map(
        functools.partial(on_device, mesh.shape["px"]),
        mesh=mesh,
        in_specs=in_specs,
        out_specs=out_specs,
        check_vma=False,
    )
```

```python
import functools
import math

import jax
import jax.numpy as jnp
import numpy as np
from jax import lax
from jax.experimental import pallas as pl
from jax.experimental.pallas import tpu as pltpu
from jax.sharding import PartitionSpec as P

KX = 32
KY = 32
KZ = 16
LANES = 128
PACK = LANES // KZ
QUAD = 4
TOP = 8
MOST = 63 << 20

TWO_PI = 2.0 * math.pi


def signed_modes(number):
    ladder = np.arange(number)
    return np.where(ladder < number // 2, ladder, ladder - number)


def phase_table(length, frequency):
    product = np.arange(length)[:, None] * frequency[None, :] % length
    return product.astype(np.float32) * np.float32(TWO_PI / length)


def rounded(table):
    return np.asarray(table).astype(jnp.bfloat16)


def split(table):
    high = rounded(table)
    return high, rounded(table - high.astype(np.float32))


def forward_table(length):
    phase = phase_table(length, signed_modes(KX))
    cosine, sine = np.cos(phase), np.sin(phase)
    return np.stack([np.stack([cosine, -sine], axis=1), np.stack([sine, cosine], axis=1)], axis=0)


def inverse_table(length):
    phase = phase_table(length, signed_modes(KX))
    cosine, sine = np.cos(phase), np.sin(phase)
    return np.stack([np.stack([cosine, sine], axis=1), np.stack([-sine, cosine], axis=1)], axis=0)


def halves(value):
    high = value.astype(jnp.bfloat16)
    return high, (value - high.astype(jnp.float32)).astype(jnp.bfloat16)


def product(left, right):
    return jnp.dot(left, right, preferred_element_type=jnp.float32)


def chosen(table, axis, width, count, which):
    place = lax.broadcasted_iota(jnp.int32, table.shape, axis) // width % count
    return jnp.where(place == which, table.astype(jnp.float32), 0.0).astype(jnp.bfloat16)


def whole(*shape):
    return pl.BlockSpec(shape, lambda *step: (0,) * len(shape))


def others(parts, act):
    me = lax.axis_index("px")

    def one(k, carry):
        act(lax.rem(me + k, parts))
        return carry

    lax.fori_loop(1, parts, one, 0)


def greet(parts):
    barrier = pltpu.get_barrier_semaphore()
    others(parts, lambda to: pl.semaphore_signal(barrier, inc=1, device_id={"px": to}))


def greeted(parts):
    pl.semaphore_wait(pltpu.get_barrier_semaphore(), parts - 1)


def share(parts, sent, out, at, sems):
    me = lax.axis_index("px")
    send, receive, local = sems

    def put(to):
        pltpu.make_async_remote_copy(
            src_ref=sent.at[to, at], dst_ref=out.at[me, at], send_sem=send, recv_sem=receive, device_id={"px": to}
        ).start()

    others(parts, put)
    pltpu.make_async_copy(sent.at[me, at], out.at[me, at], local).start()


def settle(parts, sent, out, sems):
    send, receive, local = sems
    pltpu.make_async_copy(sent.at[0], out.at[0], local).wait()
    most = pl.ds(0, parts - 1)
    every = pltpu.make_async_remote_copy(
        src_ref=sent.at[most], dst_ref=out.at[most], send_sem=send, recv_sem=receive,
        device_id={"px": lax.rem(lax.axis_index("px") + 1, parts)},
    )
    every.wait_send()
    every.wait_recv()


def spread_z(base_ref, z):
    depth = base_ref.shape[0]
    for c in range(PACK):
        z[c * depth : (c + 1) * depth] = chosen(base_ref[...], 1, KZ, PACK, c)


def plane_spectra(f_ref, z, y_ref, keep):
    groups = f_ref.shape[0] // PACK
    depth = f_ref.shape[3]
    for pair in range(0, groups, 2):
        along = [0.0, 0.0]
        for c in range(PACK):
            for n in range(2):
                along[n] += product(f_ref[(pair + n) * PACK + c, 0], z[c * depth : (c + 1) * depth])
        for n in range(2):
            g = pair + n
            high, low = halves(along[n])
            both = product(y_ref[...], high)
            rest = product(y_ref[: 2 * KY], low)
            total = both[: 2 * KY] + both[2 * KY :] + rest
            cosine, sine = total[:KY], total[KY:]
            keep(g, cosine[:, :LANES] + sine[:, LANES:])
            keep(groups + g, cosine[:, LANES:] - sine[:, :LANES])


def forward_kernel(f_ref, base_ref, y_ref, out_ref, z):
    @pl.when(pl.program_id(0) == 0)
    def start():
        spread_z(base_ref, z)

    def keep(row, value):
        out_ref[:, 0, row, :] = value

    plane_spectra(f_ref, z, y_ref, keep)


def forward_share_kernel(f_ref, base_ref, y_ref, out_ref, z, sent, send, receive, local):
    x = pl.program_id(0)
    parts, _, held_y = sent.shape[:3]

    @pl.when(x == 0)
    def start():
        greet(parts)
        spread_z(base_ref, z)

    def keep(row, value):
        sent[:, pl.ds(x, 1), :, row, :] = value.reshape(parts, 1, held_y, LANES)

    plane_spectra(f_ref, z, y_ref, keep)

    @pl.when(x == 0)
    def ready():
        greeted(parts)

    share(parts, sent, out_ref, x, (send, receive, local))

    @pl.when(x == pl.num_programs(0) - 1)
    def end():
        settle(parts, sent, out_ref, (send, receive, local))


def spectra(parts, features):
    channels, planes, height, depth = features.shape
    rows = 2 * channels // PACK
    y_phase = phase_table(height, signed_modes(KY)).T
    high, low = split(np.concatenate([np.cos(y_phase), np.sin(y_phase)], axis=0))
    z_phase = phase_table(depth, np.arange(KZ))
    base = rounded(np.concatenate([np.tile(np.cos(z_phase), (1, PACK)), np.tile(-np.sin(z_phase), (1, PACK))], axis=1))
    y_table = np.concatenate([high, low], axis=0)
    call = dict(
        grid=(planes,),
        in_specs=[
            pl.BlockSpec((channels, 1, height, depth), lambda x: (0, x, 0, 0)),
            whole(*base.shape),
            whole(*y_table.shape),
        ],
    )
    z = pltpu.VMEM((PACK * depth, 2 * LANES), jnp.bfloat16)
    if parts is None:
        kernel, shape = forward_kernel, (KY, planes, rows, LANES)
        call |= dict(
            out_specs=pl.BlockSpec((KY, 1, rows, LANES), lambda x: (0, x, 0, 0)),
            scratch_shapes=[z],
            compiler_params=pltpu.CompilerParams(vmem_limit_bytes=MOST),
            name="forward_planes",
        )
    else:
        kernel, shape = forward_share_kernel, (parts, planes, KY // parts, rows, LANES)
        call |= dict(
            out_specs=pl.BlockSpec(memory_space=pl.ANY),
            scratch_shapes=[z, pltpu.VMEM(shape, jnp.float32)] + [pltpu.SemaphoreType.DMA] * 3,
            compiler_params=pltpu.CompilerParams(vmem_limit_bytes=MOST, collective_id=0, has_side_effects=True),
            name="forward_share",
        )
    out_shape = jax.ShapeDtypeStruct(shape, jnp.float32)
    return pl.pallas_call(kernel, out_shape=out_shape, **call)(features, jnp.asarray(base), jnp.asarray(y_table))


def contract(left, right):
    return jnp.einsum("im,iom->om", left, right, precision=lax.Precision.HIGHEST)


def mix_modes(spectrum, weights):
    real_part = contract(spectrum[0], weights[0]) - contract(spectrum[1], weights[1])
    imag_part = contract(spectrum[0], weights[1]) + contract(spectrum[1], weights[0])
    return jnp.stack([real_part, imag_part])


def spectrum_table(length):
    table = np.broadcast_to(forward_table(length)[:, :, :, None, :], (2, length, 2, QUAD, KX))
    return split(table.reshape(2 * length, 2 * QUAD * KX))


def planes_table(length):
    table = inverse_table(length).transpose(0, 3, 2, 1)
    table = np.broadcast_to(table[:, None], (2, QUAD, KX, 2, length))
    return split(table.reshape(2 * QUAD * KX, 2 * length))


def modes_kernel(g_ref, fhigh_ref, flow_ref, ihigh_ref, ilow_ref, w_ref, out_ref, *scratch):
    fhigh, flow, ihigh, ilow, turned, spectrum, blended, placed, sent, send, receive, local = scratch
    parts, planes, held_y, rows, _ = g_ref.shape
    length = parts * planes
    channels = w_ref.shape[1]
    quads = KZ // QUAD
    groups = rows // 2
    here = pl.program_id(0)

    @pl.when(here == 0)
    def start():
        greet(parts)
        for q in range(QUAD):
            at = slice(q * 2 * length, (q + 1) * 2 * length)
            fhigh[at], flow[at] = chosen(fhigh_ref[...], 1, KX, QUAD, q), chosen(flow_ref[...], 1, KX, QUAD, q)
            ihigh[:, at], ilow[:, at] = chosen(ihigh_ref[...], 0, KX, QUAD, q), chosen(ilow_ref[...], 0, KX, QUAD, q)

    for j in range(held_y):

        @pl.when(here == j * quads)
        def along_x(j=j):
            for r in range(2):
                for g in range(groups):
                    tile = g_ref[:, :, j, r * groups + g, :].reshape(length, LANES)
                    turned[r, g * LANES : (g + 1) * LANES, :] = tile.T
            for b in range(quads):
                pieces = [
                    turned[r, pl.ds(b * QUAD + q, channels, stride=KZ), :] for q in range(QUAD) for r in range(2)
                ]
                high, low = halves(jnp.concatenate(pieces, axis=1))
                value = product(high, fhigh[...]) + product(high, flow[...]) + product(low, fhigh[...])
                spectrum[j * quads + b] = value

    def mix(i, total):
        real, imag = total
        row = spectrum[here, pl.ds(i, 1), :]
        s_real, s_imag = row[:, :LANES], row[:, LANES:]
        w_real, w_imag = w_ref[0, i], w_ref[1, i]
        return real + (s_real * w_real - s_imag * w_imag), imag + (s_real * w_imag + s_imag * w_real)

    zero = jnp.zeros((channels, LANES), jnp.float32)
    real, imag = lax.fori_loop(0, channels, mix, (zero, zero), unroll=4)
    blended[here, :, :LANES] = real
    blended[here, :, LANES:] = imag

    for j in range(held_y):

        @pl.when(here == (j + 1) * quads - 1)
        def back_along_x(j=j):
            high, low = halves(blended[j * quads : (j + 1) * quads].reshape(quads * channels, 2 * LANES))
            value = product(high, ihigh[...]) + product(high, ilow[...]) + product(low, ihigh[...])
            for b in range(quads):
                for q in range(QUAD):
                    for r in range(2):
                        at = (q * 2 + r) * length
                        row = pl.ds(r * KZ + b * QUAD + q, channels, stride=2 * KZ)
                        placed[j, row, :] = value[b * channels : (b + 1) * channels, at : at + length]
            for h in range(sent.shape[3]):
                tile = placed[j, h * LANES : (h + 1) * LANES, :].T
                sent[:, j, :, h, :] = tile.reshape(parts, planes, LANES)
            if j == 0:
                greeted(parts)
            share(parts, sent, out_ref, j, (send, receive, local))
            if j == held_y - 1:
                settle(parts, sent, out_ref, (send, receive, local))


def mix_on_device(gathered, spectral_weight):
    parts, planes, held_y, rows, _ = gathered.shape
    length = parts * planes
    channels = spectral_weight.shape[1]
    blocks = held_y * KZ // QUAD
    tables = (*spectrum_table(length), *planes_table(length))
    packs = channels * 2 * KZ // LANES
    shape = (parts, held_y, planes, packs, LANES)
    wide = QUAD * 2 * length
    return pl.pallas_call(
        modes_kernel,
        grid=(blocks,),
        out_shape=jax.ShapeDtypeStruct(shape, jnp.float32),
        in_specs=[whole(*gathered.shape)]
        + [whole(*table.shape) for table in tables]
        + [pl.BlockSpec((2, channels, channels, LANES), lambda b: (0, 0, 0, b))],
        out_specs=pl.BlockSpec(memory_space=pl.ANY),
        scratch_shapes=[pltpu.VMEM((wide, 2 * LANES), jnp.bfloat16)] * 2
        + [pltpu.VMEM((2 * LANES, wide), jnp.bfloat16)] * 2
        + [
            pltpu.VMEM((2, channels * KZ, length), jnp.float32),
            pltpu.VMEM((blocks, channels, 2 * LANES), jnp.float32),
            pltpu.VMEM((blocks, channels, 2 * LANES), jnp.float32),
            pltpu.VMEM((held_y, channels * 2 * KZ, length), jnp.float32),
            pltpu.VMEM(shape, jnp.float32),
        ]
        + [pltpu.SemaphoreType.DMA] * 3,
        compiler_params=pltpu.CompilerParams(vmem_limit_bytes=MOST, collective_id=1, has_side_effects=True),
        name="mix_share",
    )(gathered, *map(jnp.asarray, tables), spectral_weight)


def inverse_kernel(f_ref, q_ref, w_ref, left_ref, right_ref, zhigh_ref, zlow_ref, y_ref, bias_ref, out_ref, *scratch):
    mix, z, linear, other, waves = scratch
    channels, _, height, depth = f_ref.shape
    rows_each = height // channels
    packs = LANES // (2 * KZ)
    stacks = channels // packs
    step = pl.program_id(0)

    @pl.when(step == 0)
    def start():
        tall = product(left_ref[...], w_ref[...]).astype(jnp.bfloat16)
        wide = product(tall, right_ref[...])
        row = lax.broadcasted_iota(jnp.int32, wide.shape, 0)
        column = lax.broadcasted_iota(jnp.int32, wide.shape, 1)
        mix[...] = jnp.where(row % rows_each == column % rows_each, 0.5 * wide, 0.0).astype(jnp.bfloat16)
        z[: 2 * KZ] = zhigh_ref[...]
        z[2 * KZ : 4 * KZ] = zhigh_ref[...]
        z[4 * KZ : 6 * KZ] = zlow_ref[...]
        z[6 * KZ :] = jnp.zeros((LANES - 6 * KZ, 2 * depth), jnp.bfloat16)

    def along_z():
        modes = jnp.concatenate([q_ref[:, :, 0, h, :].reshape(KY, LANES) for h in range(stacks)], axis=0)
        high = modes.astype(jnp.bfloat16).astype(jnp.float32)
        low = modes - high
        lane = lax.broadcasted_iota(jnp.int32, modes.shape, 1) // (2 * KZ)
        first = lax.broadcasted_iota(jnp.int32, (TOP, depth), 0) == 0
        for k in range(packs):
            turned = lambda value, to: pltpu.roll(value, (to - k) * 2 * KZ % LANES, 1)
            left = jnp.where(lane == 0, turned(high, 0), jnp.where(lane == 1, turned(low, 1), turned(high, 2)))
            value = product(jnp.where(lane < 3, left, 0.0).astype(jnp.bfloat16), z[...])
            for h in range(stacks):
                c = h * packs + k
                part = value[h * KY : (h + 1) * KY]
                top = part[:TOP, :depth] + jnp.where(first, 0.5 * bias_ref[c], 0.0)
                real = jnp.concatenate([top, part[TOP:, :depth]], axis=0)
                imag = part[:, depth:]
                waves[c, :KY], waves[c, 2 * KY : 3 * KY] = halves(real)
                waves[c, KY : 2 * KY], waves[c, 3 * KY :] = halves(imag)

    def pointwise(t, into):
        rows = pl.ds(t * rows_each if isinstance(t, int) else pl.multiple_of(t * rows_each, rows_each), rows_each)
        local = f_ref[:, 0, rows, :].reshape(height, depth)
        into[:, rows, :] = product(mix[...], local).reshape(channels, rows_each, depth)

    def finish(c, held):
        wave = waves[c]
        stack = jnp.concatenate([wave, wave[: 2 * KY]], axis=0)
        half = product(y_ref[...], stack) + held[c]
        inner = half * (2.0 * 0.7978845608 + (8.0 * 0.7978845608 * 0.044715) * (half * half))
        out_ref[c, 0] = (half + half * jnp.tanh(inner)).astype(jnp.bfloat16)

    def work(into, held):
        @pl.when(step == 0)
        def first():
            lax.fori_loop(0, channels, lambda t, carry: (pointwise(t, into), carry)[1], 0, unroll=8)

        @pl.when(step == pl.num_programs(0) - 1)
        def last():
            along_z()
            lax.fori_loop(0, channels, lambda t, carry: (finish(t, held), carry)[1], 0, unroll=8)

        @pl.when((step > 0) & (step < pl.num_programs(0) - 1))
        def middle():
            along_z()

            for t in range(channels):
                pointwise(t, into)
                finish(t, held)

    @pl.when(step % 2 == 0)
    def even():
        work(linear, other)

    @pl.when(step % 2 == 1)
    def odd():
        work(other, linear)


def finish_planes(modes, features, pointwise_weight, pointwise_bias, cells):
    channels, planes, height, depth = features.shape
    owners, held_y, _, stacks, _ = modes.shape
    y_phase = phase_table(height, signed_modes(KY))
    high, low = split(np.concatenate([np.cos(y_phase), -np.sin(y_phase)], axis=1))
    y_table = np.concatenate([high, high, low], axis=1)
    z_phase = phase_table(depth, np.arange(KZ)).T
    factor = (0.5 * np.where(np.arange(KZ) == 0, 1.0, 2.0) / cells).astype(np.float32)[:, None]
    cosine, sine = factor * np.cos(z_phase), factor * np.sin(z_phase)
    z_high, z_low = split(np.block([[cosine, sine], [-sine, cosine]]))
    left = rounded(np.repeat(np.eye(channels, dtype=np.float32), height // channels, axis=0))
    plane = (channels, 1, height, depth)
    return pl.pallas_call(
        inverse_kernel,
        grid=(planes + 1,),
        out_shape=jax.ShapeDtypeStruct(features.shape, jnp.bfloat16),
        in_specs=[
            pl.BlockSpec(plane, lambda x: (0, jnp.minimum(x, planes - 1), 0, 0)),
            pl.BlockSpec((owners, held_y, 1, stacks, LANES), lambda x: (0, 0, jnp.maximum(x - 1, 0), 0, 0)),
            whole(channels, channels),
            whole(height, channels),
            whole(channels, height),
            whole(*z_high.shape),
            whole(*z_low.shape),
            whole(*y_table.shape),
            pl.BlockSpec(memory_space=pltpu.SMEM),
        ],
        out_specs=pl.BlockSpec(plane, lambda x: (0, jnp.maximum(x - 1, 0), 0, 0)),
        scratch_shapes=[
            pltpu.VMEM((height, height), jnp.bfloat16),
            pltpu.VMEM((LANES, 2 * depth), jnp.bfloat16),
            pltpu.VMEM((channels, height, depth), jnp.float32),
            pltpu.VMEM((channels, height, depth), jnp.float32),
            pltpu.VMEM((channels, 4 * KY, depth), jnp.bfloat16),
        ],
        compiler_params=pltpu.CompilerParams(vmem_limit_bytes=MOST),
        name="inverse_planes",
    )(
        features, modes, pointwise_weight, jnp.asarray(left), jnp.asarray(left.T), jnp.asarray(z_high),
        jnp.asarray(z_low), jnp.asarray(y_table), pointwise_bias,
    )


def by_einsum(parts, features, spectral_weight):
    channels, planes, height, depth = features.shape
    length = planes * parts
    held_y = max(KY // parts, 1)
    cuts = parts * held_y // KY
    held_z = KZ // cuts
    packs = LANES // (2 * KZ)
    exact = functools.partial(jnp.einsum, precision=lax.Precision.HIGHEST)
    exchange = functools.partial(lax.all_to_all, axis_name="px", split_axis=0, concat_axis=0, tiled=True)

    sent = spectra(None, features)
    sent = sent.reshape(KY, planes, 2 * channels, cuts, held_z).transpose(0, 3, 1, 2, 4)
    sent = sent.reshape(parts, held_y * planes * 2 * channels * held_z // LANES, LANES)
    gathered = exchange(sent).reshape(parts, held_y, planes, 2, channels, held_z)
    table = jnp.asarray(forward_table(length).reshape(2, parts, planes, 2, KX))
    spectrum = exact("sjprck,rsptm->tcjkm", gathered, table)
    blended = mix_modes(spectrum.reshape(2, channels, held_y * held_z * KX), spectral_weight)
    blended = blended.reshape(2, channels, held_y, held_z, KX)
    table = jnp.asarray(inverse_table(length).reshape(2, parts, planes, 2, KX))
    sent = exact("rcjkm,rsptm->spjtck", blended, table)
    sent = sent.reshape(parts, held_y * planes * 2 * channels * held_z // LANES, LANES)
    spread = exchange(sent).reshape(KY // held_y, cuts, planes, held_y, 2, channels // packs, packs, held_z)
    modes = spread.transpose(0, 3, 2, 5, 6, 4, 1, 7)
    return modes.reshape(KY // held_y, held_y, planes, channels // packs, LANES)


def on_device(parts, features, pointwise_weight, pointwise_bias, spectral_weight):
    channels, planes, height, depth = features.shape
    length = planes * parts
    if KY % parts == 0 and length == LANES:
        modes = mix_on_device(spectra(parts, features), spectral_weight)
    else:
        modes = by_einsum(parts, features, spectral_weight)
    return finish_planes(
        modes, features, pointwise_weight, pointwise_bias, 1.0 * length * height * depth
    )


def solution(mesh):
    in_specs = (P(None, ("groups", "px"), None, None), P(), P(), P(None, None, None, "px"))
    out_specs = P(None, ("groups", "px"), None, None)
    return jax.shard_map(
        functools.partial(on_device, mesh.shape["px"]),
        mesh=mesh,
        in_specs=in_specs,
        out_specs=out_specs,
        check_vma=False,
    )
```

```python
import functools
import math

import jax
import jax.numpy as jnp
import numpy as np
from jax import lax
from jax.experimental import pallas as pl
from jax.experimental.pallas import tpu as pltpu
from jax.sharding import PartitionSpec as P

KX = 32
KY = 32
KZ = 16
LANES = 128
PACK = LANES // KZ
QUAD = 4
TOP = 8
MOST = 63 << 20

TWO_PI = 2.0 * math.pi


def signed_modes(number):
    ladder = np.arange(number)
    return np.where(ladder < number // 2, ladder, ladder - number)


def phase_table(length, frequency):
    product = np.arange(length)[:, None] * frequency[None, :] % length
    return product.astype(np.float32) * np.float32(TWO_PI / length)


def rounded(table):
    return np.asarray(table).astype(jnp.bfloat16)


def split(table):
    high = rounded(table)
    return high, rounded(table - high.astype(np.float32))


def forward_table(length):
    phase = phase_table(length, signed_modes(KX))
    cosine, sine = np.cos(phase), np.sin(phase)
    return np.stack([np.stack([cosine, -sine], axis=1), np.stack([sine, cosine], axis=1)], axis=0)


def inverse_table(length):
    phase = phase_table(length, signed_modes(KX))
    cosine, sine = np.cos(phase), np.sin(phase)
    return np.stack([np.stack([cosine, sine], axis=1), np.stack([-sine, cosine], axis=1)], axis=0)


def halves(value):
    high = value.astype(jnp.bfloat16)
    return high, (value - high.astype(jnp.float32)).astype(jnp.bfloat16)


def product(left, right):
    return jnp.dot(left, right, preferred_element_type=jnp.float32)


def chosen(table, axis, width, count, which):
    place = lax.broadcasted_iota(jnp.int32, table.shape, axis) // width % count
    return jnp.where(place == which, table.astype(jnp.float32), 0.0).astype(jnp.bfloat16)


def whole(*shape):
    return pl.BlockSpec(shape, lambda *step: (0,) * len(shape))


def others(parts, act):
    me = lax.axis_index("px")

    def one(k, carry):
        act(lax.rem(me + k, parts))
        return carry

    lax.fori_loop(1, parts, one, 0)


def greet(parts):
    barrier = pltpu.get_barrier_semaphore()
    others(parts, lambda to: pl.semaphore_signal(barrier, inc=1, device_id={"px": to}))


def greeted(parts):
    pl.semaphore_wait(pltpu.get_barrier_semaphore(), parts - 1)


def share(parts, sent, out, at, sems):
    me = lax.axis_index("px")
    send, receive, local = sems

    def put(to):
        pltpu.make_async_remote_copy(
            src_ref=sent.at[to, at], dst_ref=out.at[me, at], send_sem=send, recv_sem=receive, device_id={"px": to}
        ).start()

    others(parts, put)
    pltpu.make_async_copy(sent.at[me, at], out.at[me, at], local).start()


def settle(parts, sent, out, sems):
    send, receive, local = sems
    pltpu.make_async_copy(sent.at[0], out.at[0], local).wait()
    most = pl.ds(0, parts - 1)
    every = pltpu.make_async_remote_copy(
        src_ref=sent.at[most], dst_ref=out.at[most], send_sem=send, recv_sem=receive,
        device_id={"px": lax.rem(lax.axis_index("px") + 1, parts)},
    )
    every.wait_send()
    every.wait_recv()


def spread_z(base_ref, z):
    depth = base_ref.shape[0]
    for c in range(PACK):
        z[c * depth : (c + 1) * depth] = chosen(base_ref[...], 1, KZ, PACK, c)


def plane_spectra(f_ref, z, y_ref, keep):
    groups = f_ref.shape[0] // PACK
    depth = f_ref.shape[3]
    for pair in range(0, groups, 2):
        along = [0.0, 0.0]
        for c in range(PACK):
            for n in range(2):
                along[n] += product(f_ref[(pair + n) * PACK + c, 0], z[c * depth : (c + 1) * depth])
        for n in range(2):
            g = pair + n
            high, low = halves(along[n])
            both = product(y_ref[...], high)
            rest = product(y_ref[: 2 * KY], low)
            total = both[: 2 * KY] + both[2 * KY :] + rest
            cosine, sine = total[:KY], total[KY:]
            keep(g, cosine[:, :LANES] + sine[:, LANES:])
            keep(groups + g, cosine[:, LANES:] - sine[:, :LANES])


def forward_kernel(f_ref, base_ref, y_ref, out_ref, z):
    @pl.when(pl.program_id(0) == 0)
    def start():
        spread_z(base_ref, z)

    def keep(row, value):
        out_ref[:, 0, row, :] = value

    plane_spectra(f_ref, z, y_ref, keep)


def forward_share_kernel(f_ref, base_ref, y_ref, out_ref, z, sent, send, receive, local):
    x = pl.program_id(0)
    parts, _, held_y = sent.shape[:3]

    @pl.when(x == 0)
    def start():
        greet(parts)
        spread_z(base_ref, z)

    def keep(row, value):
        sent[:, pl.ds(x, 1), :, row, :] = value.reshape(parts, 1, held_y, LANES)

    plane_spectra(f_ref, z, y_ref, keep)

    @pl.when(x == 0)
    def ready():
        greeted(parts)

    share(parts, sent, out_ref, x, (send, receive, local))

    @pl.when(x == pl.num_programs(0) - 1)
    def end():
        settle(parts, sent, out_ref, (send, receive, local))


def spectra(parts, features):
    channels, planes, height, depth = features.shape
    rows = 2 * channels // PACK
    y_phase = phase_table(height, signed_modes(KY)).T
    high, low = split(np.concatenate([np.cos(y_phase), np.sin(y_phase)], axis=0))
    z_phase = phase_table(depth, np.arange(KZ))
    base = rounded(np.concatenate([np.tile(np.cos(z_phase), (1, PACK)), np.tile(-np.sin(z_phase), (1, PACK))], axis=1))
    y_table = np.concatenate([high, low], axis=0)
    call = dict(
        grid=(planes,),
        in_specs=[
            pl.BlockSpec((channels, 1, height, depth), lambda x: (0, x, 0, 0)),
            whole(*base.shape),
            whole(*y_table.shape),
        ],
    )
    z = pltpu.VMEM((PACK * depth, 2 * LANES), jnp.bfloat16)
    if parts is None:
        kernel, shape = forward_kernel, (KY, planes, rows, LANES)
        call |= dict(
            out_specs=pl.BlockSpec((KY, 1, rows, LANES), lambda x: (0, x, 0, 0)),
            scratch_shapes=[z],
            compiler_params=pltpu.CompilerParams(vmem_limit_bytes=MOST),
            name="forward_planes",
        )
    else:
        kernel, shape = forward_share_kernel, (parts, planes, KY // parts, rows, LANES)
        call |= dict(
            out_specs=pl.BlockSpec(memory_space=pl.ANY),
            scratch_shapes=[z, pltpu.VMEM(shape, jnp.float32)] + [pltpu.SemaphoreType.DMA] * 3,
            compiler_params=pltpu.CompilerParams(vmem_limit_bytes=MOST, collective_id=0, has_side_effects=True),
            name="forward_share",
        )
    out_shape = jax.ShapeDtypeStruct(shape, jnp.float32)
    return pl.pallas_call(kernel, out_shape=out_shape, **call)(features, jnp.asarray(base), jnp.asarray(y_table))


def contract(left, right):
    return jnp.einsum("im,iom->om", left, right, precision=lax.Precision.HIGHEST)


def mix_modes(spectrum, weights):
    real_part = contract(spectrum[0], weights[0]) - contract(spectrum[1], weights[1])
    imag_part = contract(spectrum[0], weights[1]) + contract(spectrum[1], weights[0])
    return jnp.stack([real_part, imag_part])


def spectrum_table(length):
    table = np.broadcast_to(forward_table(length)[:, :, :, None, :], (2, length, 2, QUAD, KX))
    return split(table.reshape(2 * length, 2 * QUAD * KX))


def planes_table(length):
    table = inverse_table(length).transpose(0, 3, 2, 1)
    table = np.broadcast_to(table[:, None], (2, QUAD, KX, 2, length))
    return split(table.reshape(2 * QUAD * KX, 2 * length))


def modes_kernel(g_ref, fhigh_ref, flow_ref, ihigh_ref, ilow_ref, wreal_ref, wimag_ref, out_ref, *scratch):
    fhigh, flow, ihigh, ilow, turned, spectrum, blended, placed, sent, send, receive, local = scratch
    parts, planes, held_y, rows, _ = g_ref.shape
    length = parts * planes
    channels = wreal_ref.shape[1]
    quads = KZ // QUAD
    groups = rows // 2
    here = pl.program_id(0)

    @pl.when(here == 0)
    def start():
        greet(parts)
        for q in range(QUAD):
            at = slice(q * 2 * length, (q + 1) * 2 * length)
            fhigh[at], flow[at] = chosen(fhigh_ref[...], 1, KX, QUAD, q), chosen(flow_ref[...], 1, KX, QUAD, q)

    for j in range(held_y):

        @pl.when(here == j * quads)
        def along_x(j=j):
            for r in range(2):
                for g in range(groups):
                    tile = g_ref[:, :, j, r * groups + g, :].reshape(length, LANES)
                    turned[r, g * LANES : (g + 1) * LANES, :] = tile.T
            for b in range(quads):
                pieces = [
                    turned[r, pl.ds(b * QUAD + q, channels, stride=KZ), :] for q in range(QUAD) for r in range(2)
                ]
                high, low = halves(jnp.concatenate(pieces, axis=1))
                value = product(high, fhigh[...]) + product(high, flow[...]) + product(low, fhigh[...])
                spectrum[j * quads + b] = value

    def mix(i, total):
        real, imag = total
        row = spectrum[here, pl.ds(i, 1), :]
        s_real, s_imag = row[:, :LANES], row[:, LANES:]
        w_real, w_imag = wreal_ref[0, i], wimag_ref[0, i]
        return real + (s_real * w_real - s_imag * w_imag), imag + (s_real * w_imag + s_imag * w_real)

    @pl.when(here == 1)
    def widen():
        for q in range(QUAD):
            at = slice(q * 2 * length, (q + 1) * 2 * length)
            ihigh[:, at], ilow[:, at] = chosen(ihigh_ref[...], 0, KX, QUAD, q), chosen(ilow_ref[...], 0, KX, QUAD, q)

    zero = jnp.zeros((channels, LANES), jnp.float32)
    real, imag = lax.fori_loop(0, channels, mix, (zero, zero), unroll=8)
    blended[here, :, :LANES] = real
    blended[here, :, LANES:] = imag

    for j in range(held_y):

        @pl.when(here == (j + 1) * quads - 1)
        def back_along_x(j=j):
            high, low = halves(blended[j * quads : (j + 1) * quads].reshape(quads * channels, 2 * LANES))
            value = product(high, ihigh[...]) + product(high, ilow[...]) + product(low, ihigh[...])
            for b in range(quads):
                for q in range(QUAD):
                    for r in range(2):
                        at = (q * 2 + r) * length
                        row = pl.ds(r * KZ + b * QUAD + q, channels, stride=2 * KZ)
                        placed[j, row, :] = value[b * channels : (b + 1) * channels, at : at + length]
            for h in range(sent.shape[3]):
                tile = placed[j, h * LANES : (h + 1) * LANES, :].T
                sent[:, j, :, h, :] = tile.reshape(parts, planes, LANES)
            if j == 0:
                greeted(parts)
            share(parts, sent, out_ref, j, (send, receive, local))
            if j == held_y - 1:
                settle(parts, sent, out_ref, (send, receive, local))


def mix_on_device(gathered, spectral_weight):
    parts, planes, held_y, rows, _ = gathered.shape
    length = parts * planes
    channels = spectral_weight.shape[1]
    blocks = held_y * KZ // QUAD
    tables = (*spectrum_table(length), *planes_table(length))
    packs = channels * 2 * KZ // LANES
    shape = (parts, held_y, planes, packs, LANES)
    wide = QUAD * 2 * length
    return pl.pallas_call(
        modes_kernel,
        grid=(blocks,),
        out_shape=jax.ShapeDtypeStruct(shape, jnp.float32),
        in_specs=[whole(*gathered.shape)]
        + [whole(*table.shape) for table in tables]
        + [pl.BlockSpec((1, channels, channels, LANES), lambda b, part=part: (part, 0, 0, b)) for part in range(2)],
        out_specs=pl.BlockSpec(memory_space=pl.ANY),
        scratch_shapes=[pltpu.VMEM((wide, 2 * LANES), jnp.bfloat16)] * 2
        + [pltpu.VMEM((2 * LANES, wide), jnp.bfloat16)] * 2
        + [
            pltpu.VMEM((2, channels * KZ, length), jnp.float32),
            pltpu.VMEM((blocks, channels, 2 * LANES), jnp.float32),
            pltpu.VMEM((blocks, channels, 2 * LANES), jnp.float32),
            pltpu.VMEM((held_y, channels * 2 * KZ, length), jnp.float32),
            pltpu.VMEM(shape, jnp.float32),
        ]
        + [pltpu.SemaphoreType.DMA] * 3,
        compiler_params=pltpu.CompilerParams(vmem_limit_bytes=MOST, collective_id=1, has_side_effects=True),
        name="mix_share",
    )(gathered, *map(jnp.asarray, tables), spectral_weight, spectral_weight)


def inverse_kernel(f_ref, q_ref, w_ref, left_ref, right_ref, zhigh_ref, zlow_ref, y_ref, bias_ref, out_ref, *scratch):
    mix, z, linear, other, waves = scratch
    channels, _, height, depth = f_ref.shape
    rows_each = height // channels
    packs = LANES // (2 * KZ)
    stacks = channels // packs
    step = pl.program_id(0)

    @pl.when(step == 0)
    def start():
        tall = product(left_ref[...], w_ref[...]).astype(jnp.bfloat16)
        wide = product(tall, right_ref[...])
        row = lax.broadcasted_iota(jnp.int32, wide.shape, 0)
        column = lax.broadcasted_iota(jnp.int32, wide.shape, 1)
        mix[...] = jnp.where(row % rows_each == column % rows_each, 0.5 * wide, 0.0).astype(jnp.bfloat16)
        z[: 2 * KZ] = zhigh_ref[...]
        z[2 * KZ : 4 * KZ] = zhigh_ref[...]
        z[4 * KZ : 6 * KZ] = zlow_ref[...]
        z[6 * KZ :] = jnp.zeros((LANES - 6 * KZ, 2 * depth), jnp.bfloat16)

    def along_z():
        modes = jnp.concatenate([q_ref[:, :, 0, h, :].reshape(KY, LANES) for h in range(stacks)], axis=0)
        high = modes.astype(jnp.bfloat16).astype(jnp.float32)
        low = modes - high
        lane = lax.broadcasted_iota(jnp.int32, modes.shape, 1) // (2 * KZ)
        first = lax.broadcasted_iota(jnp.int32, (TOP, depth), 0) == 0
        for k in range(packs):
            turned = lambda value, to: pltpu.roll(value, (to - k) * 2 * KZ % LANES, 1)
            left = jnp.where(lane == 0, turned(high, 0), jnp.where(lane == 1, turned(low, 1), turned(high, 2)))
            value = product(jnp.where(lane < 3, left, 0.0).astype(jnp.bfloat16), z[...])
            for h in range(stacks):
                c = h * packs + k
                part = value[h * KY : (h + 1) * KY]
                top = part[:TOP, :depth] + jnp.where(first, 0.5 * bias_ref[c], 0.0)
                real = jnp.concatenate([top, part[TOP:, :depth]], axis=0)
                imag = part[:, depth:]
                waves[c, :KY], waves[c, 2 * KY : 3 * KY] = halves(real)
                waves[c, KY : 2 * KY], waves[c, 3 * KY :] = halves(imag)

    def pointwise(t, into):
        rows = pl.ds(t * rows_each if isinstance(t, int) else pl.multiple_of(t * rows_each, rows_each), rows_each)
        local = f_ref[:, 0, rows, :].reshape(height, depth)
        into[:, rows, :] = product(mix[...], local).reshape(channels, rows_each, depth)

    def finish(c, held):
        wave = waves[c]
        stack = jnp.concatenate([wave, wave[: 2 * KY]], axis=0)
        half = product(y_ref[...], stack) + held[c]
        inner = half * (2.0 * 0.7978845608 + (8.0 * 0.7978845608 * 0.044715) * (half * half))
        out_ref[c, 0] = (half + half * jnp.tanh(inner)).astype(jnp.bfloat16)

    def work(into, held):
        @pl.when(step == 0)
        def first():
            lax.fori_loop(0, channels, lambda t, carry: (pointwise(t, into), carry)[1], 0, unroll=8)

        @pl.when(step == pl.num_programs(0) - 1)
        def last():
            along_z()
            lax.fori_loop(0, channels, lambda t, carry: (finish(t, held), carry)[1], 0, unroll=8)

        @pl.when((step > 0) & (step < pl.num_programs(0) - 1))
        def middle():
            along_z()

            for t in range(channels):
                pointwise(t, into)
                finish(t, held)

    @pl.when(step % 2 == 0)
    def even():
        work(linear, other)

    @pl.when(step % 2 == 1)
    def odd():
        work(other, linear)


def finish_planes(modes, features, pointwise_weight, pointwise_bias, cells):
    channels, planes, height, depth = features.shape
    owners, held_y, _, stacks, _ = modes.shape
    y_phase = phase_table(height, signed_modes(KY))
    high, low = split(np.concatenate([np.cos(y_phase), -np.sin(y_phase)], axis=1))
    y_table = np.concatenate([high, high, low], axis=1)
    z_phase = phase_table(depth, np.arange(KZ)).T
    factor = (0.5 * np.where(np.arange(KZ) == 0, 1.0, 2.0) / cells).astype(np.float32)[:, None]
    cosine, sine = factor * np.cos(z_phase), factor * np.sin(z_phase)
    z_high, z_low = split(np.block([[cosine, sine], [-sine, cosine]]))
    left = rounded(np.repeat(np.eye(channels, dtype=np.float32), height // channels, axis=0))
    plane = (channels, 1, height, depth)
    return pl.pallas_call(
        inverse_kernel,
        grid=(planes + 1,),
        out_shape=jax.ShapeDtypeStruct(features.shape, jnp.bfloat16),
        in_specs=[
            pl.BlockSpec(plane, lambda x: (0, jnp.minimum(x, planes - 1), 0, 0)),
            pl.BlockSpec((owners, held_y, 1, stacks, LANES), lambda x: (0, 0, jnp.maximum(x - 1, 0), 0, 0)),
            whole(channels, channels),
            whole(height, channels),
            whole(channels, height),
            whole(*z_high.shape),
            whole(*z_low.shape),
            whole(*y_table.shape),
            pl.BlockSpec(memory_space=pltpu.SMEM),
        ],
        out_specs=pl.BlockSpec(plane, lambda x: (0, jnp.maximum(x - 1, 0), 0, 0)),
        scratch_shapes=[
            pltpu.VMEM((height, height), jnp.bfloat16),
            pltpu.VMEM((LANES, 2 * depth), jnp.bfloat16),
            pltpu.VMEM((channels, height, depth), jnp.float32),
            pltpu.VMEM((channels, height, depth), jnp.float32),
            pltpu.VMEM((channels, 4 * KY, depth), jnp.bfloat16),
        ],
        compiler_params=pltpu.CompilerParams(vmem_limit_bytes=MOST),
        name="inverse_planes",
    )(
        features, modes, pointwise_weight, jnp.asarray(left), jnp.asarray(left.T), jnp.asarray(z_high),
        jnp.asarray(z_low), jnp.asarray(y_table), pointwise_bias,
    )


def by_einsum(parts, features, spectral_weight):
    channels, planes, height, depth = features.shape
    length = planes * parts
    held_y = max(KY // parts, 1)
    cuts = parts * held_y // KY
    held_z = KZ // cuts
    packs = LANES // (2 * KZ)
    exact = functools.partial(jnp.einsum, precision=lax.Precision.HIGHEST)
    exchange = functools.partial(lax.all_to_all, axis_name="px", split_axis=0, concat_axis=0, tiled=True)

    sent = spectra(None, features)
    sent = sent.reshape(KY, planes, 2 * channels, cuts, held_z).transpose(0, 3, 1, 2, 4)
    sent = sent.reshape(parts, held_y * planes * 2 * channels * held_z // LANES, LANES)
    gathered = exchange(sent).reshape(parts, held_y, planes, 2, channels, held_z)
    table = jnp.asarray(forward_table(length).reshape(2, parts, planes, 2, KX))
    spectrum = exact("sjprck,rsptm->tcjkm", gathered, table)
    blended = mix_modes(spectrum.reshape(2, channels, held_y * held_z * KX), spectral_weight)
    blended = blended.reshape(2, channels, held_y, held_z, KX)
    table = jnp.asarray(inverse_table(length).reshape(2, parts, planes, 2, KX))
    sent = exact("rcjkm,rsptm->spjtck", blended, table)
    sent = sent.reshape(parts, held_y * planes * 2 * channels * held_z // LANES, LANES)
    spread = exchange(sent).reshape(KY // held_y, cuts, planes, held_y, 2, channels // packs, packs, held_z)
    modes = spread.transpose(0, 3, 2, 5, 6, 4, 1, 7)
    return modes.reshape(KY // held_y, held_y, planes, channels // packs, LANES)


def on_device(parts, features, pointwise_weight, pointwise_bias, spectral_weight):
    channels, planes, height, depth = features.shape
    length = planes * parts
    if KY % parts == 0 and length == LANES:
        modes = mix_on_device(spectra(parts, features), spectral_weight)
    else:
        modes = by_einsum(parts, features, spectral_weight)
    return finish_planes(
        modes, features, pointwise_weight, pointwise_bias, 1.0 * length * height * depth
    )


def solution(mesh):
    in_specs = (P(None, ("groups", "px"), None, None), P(), P(), P(None, None, None, "px"))
    out_specs = P(None, ("groups", "px"), None, None)
    return jax.shard_map(
        functools.partial(on_device, mesh.shape["px"]),
        mesh=mesh,
        in_specs=in_specs,
        out_specs=out_specs,
        check_vma=False,
    )
```
